32 devices in a mesh: groups: 2 (over y), batch: 4 (over z), blk: 4 (over x, core).
Axes of the slice: x: 2, y: 2, z: 4, core: 2. Of those that a mesh axis runs over, the one named last changes fastest.
Arguments:
- queries: bfloat16 [8, 592, 1024], P(('groups', 'batch'), 'blk'), parts along dimension 0, may hold values from -12 to 12
- key_states: bfloat16 [8, 592, 1024], P(('groups', 'batch'), 'blk'), parts along dimension 0, may hold values from -6 to 6
- value_states: bfloat16 [8, 592, 1024], P(('groups', 'batch'), 'blk'), parts along dimension 0, may hold values from -6 to 6
- residual: bfloat16 [8, 592, 768], P(('groups', 'batch'), 'blk'), parts along dimension 0, may hold values from -3 to 3
- proj_weight: bfloat16 [1024, 768], P(None, 'batch'), may hold values from -0.1875 to 0.1875
- conv_weight: bfloat16 [3, 3, 768, 384], P(None, None, 'batch'), may hold values from -0.078125 to 0.078125
Outputs:
- conv_out: bfloat16 [8, 592, 384], P(('groups', 'batch'), 'blk'), parts along dimension 0
The draws below stay inside these ranges and needn't reach their ends.
There are 2 independent parts, one for each index of `groups`. The reference program is written for one: setup_inputs(seed, part) draws one part's arguments, and reference() takes and returns one part's arrays. A program takes and returns all parts, laid end to end along the dimension named above; an argument that names none is the same for every part. Nothing has to cross between parts.
All inputs are finite; a program needn't handle non-finite values.
Results may differ from the reference program's by a relative error of at most 0.0085.
Values may be sent and summed in bfloat16 or wider, within the bound.
A program may use at most 64 MiB of HBM per device.

```python
import jax
import jax.numpy as jnp
from jax import lax

HEADS = 16
HD = 64
FEATW = 768
FEAT = 384
COLS = 74
NROWS = 8
TOKENS = 592
IMAGES = 4


def draw_queries(key, part):
    base_draw = 3.0 * jnp.clip(jax.random.normal(jax.random.fold_in(key, 1), (IMAGES, TOKENS, HEADS * HD), jnp.float32), -4.0, 4.0)
    return base_draw.astype(jnp.bfloat16)


def draw_key_states(key, part):
    base_draw = jnp.clip(jax.random.normal(jax.random.fold_in(key, 2), (IMAGES, TOKENS, HEADS * HD), jnp.float32), -6.0, 6.0)
    return base_draw.astype(jnp.bfloat16)


def levels(key, shape, shards, low, largest):
    level, own = 1.0, jax.random.fold_in(key, 6)
    for position, blocks in shards:
        steps = jnp.exp(jax.random.uniform(jax.random.fold_in(own, position), (blocks,), jnp.float32, low / len(shards), largest / len(shards)))
        level = level * jnp.repeat(steps, shape[position] // blocks).reshape([-1 if axis == position else 1 for axis in range(len(shape))])
    return level


def gaussian(rng, dims, deviation, bound, pieces=(), kind=jnp.bfloat16):
    result = jax.random.normal(rng, dims, jnp.float32) * deviation
    if len(pieces) > 0:
        result = levels(rng, dims, pieces, -0.22, 0.18) * result
    return jnp.clip(result, min=-bound, max=bound).astype(kind)


def setup_inputs(seed: int = 0, part: int = 0) -> dict:
    key_of = jax.random.split(jax.random.key(seed), 7)
    part_keys = jax.random.split(jax.random.fold_in(key_of[6], part), 7)
    queries = draw_queries(jax.random.fold_in(jax.random.fold_in(key_of[6], part), 71), part)
    key_states = draw_key_states(jax.random.fold_in(jax.random.fold_in(key_of[6], part), 71), part)
    value_states = gaussian(part_keys[2], (IMAGES, TOKENS, HEADS * HD), 1.0, 6.0, ((0, 4), (1, 4)))
    residual = gaussian(part_keys[3], (IMAGES, TOKENS, FEATW), 0.5, 3.0, ((0, 4), (1, 4)))
    proj_weight = gaussian(key_of[4], (HEADS * HD, FEATW), (HEADS * HD) ** -0.5, 0.1875, ((1, 4),))
    conv_weight = gaussian(key_of[5], (3, 3, FEATW, FEAT), (9 * FEATW) ** -0.5, 0.078125, ((2, 4),))
    return dict(queries=queries, key_states=key_states, value_states=value_states, residual=residual, proj_weight=proj_weight, conv_weight=conv_weight)


def one_head(head_args):
    query_head, key_head, value_head = head_args
    scores = jnp.dot(query_head, key_head.T, preferred_element_type=jnp.float32) * (HD ** -0.5)
    row_max = jnp.max(scores, axis=1, keepdims=True)
    weights = jnp.exp(scores - row_max)
    weight_sum = jnp.sum(weights, axis=1, keepdims=True)
    mixed = jnp.dot(weights.astype(jnp.bfloat16), value_head, preferred_element_type=jnp.float32)
    return mixed / weight_sum


def one_image(image_args, proj_weight, conv_weight):
    queries, key_states, value_states, residual = image_args
    query_heads = queries.reshape(TOKENS, HEADS, HD).transpose(1, 0, 2)
    key_heads = key_states.reshape(TOKENS, HEADS, HD).transpose(1, 0, 2)
    value_heads = value_states.reshape(TOKENS, HEADS, HD).transpose(1, 0, 2)
    mixed = lax.map(one_head, (query_heads, key_heads, value_heads))
    attention = mixed.transpose(1, 0, 2).reshape(TOKENS, HEADS * HD).astype(jnp.bfloat16)
    projected = jnp.dot(attention, proj_weight, preferred_element_type=jnp.float32)
    hidden = (residual.astype(jnp.float32) + projected).astype(jnp.bfloat16)
    feature_grid = hidden.reshape(NROWS, COLS, FEATW)
    padded = jnp.pad(feature_grid, ((1, 1), (1, 1), (0, 0)))
    conv_sum = jnp.zeros((TOKENS, FEAT), jnp.float32)
    for row_off in range(3):
        for col_off in range(3):
            window = padded[row_off:row_off + NROWS, col_off:col_off + COLS].reshape(TOKENS, FEATW)
            conv_sum = conv_sum + jnp.dot(window, conv_weight[row_off, col_off], preferred_element_type=jnp.float32)
    return conv_sum.astype(jnp.bfloat16)


def reference(queries, key_states, value_states, residual, proj_weight, conv_weight):
    return lax.map(lambda image_args: one_image(image_args, proj_weight, conv_weight),
                   (queries, key_states, value_states, residual))
```

```python
import functools

import jax
import jax.numpy as jnp
from jax import lax
from jax.experimental import pallas as pl
from jax.experimental.pallas import tpu as pltpu
from jax.sharding import PartitionSpec as P

HEADS = 16
HD = 64
COLS = 74
BASE = 8
MESH = pl.DeviceIdType.MESH


def kernel(G, Z, B, CI, NC, q_hbm, k_hbm, v_hbm, r_hbm, p_hbm, c_hbm, o_ref,
           q, res, kb, vb, wp, wc, att, hext, h_top, h_bot, r_top, r_bot, acc,
           lsem, ksend, krecv, kcs, kcr, zup, zdn, zrecv, ysend, yrecv, csend, crecv, hsend, hrecv):
    T = q.shape[0]
    X = B // 2
    g = lax.axis_index("groups")
    z = lax.axis_index("batch")
    b = lax.axis_index("blk")
    c = lax.rem(b, 2)
    x = b // 2
    mate = x * 2 + 1 - c
    NI = 1 + NC
    PP = wp.shape[1] // (2 * G)
    PC = wc.shape[1] // (2 * G)
    CC = PC // NC

    locals_ = [
        pltpu.make_async_copy(k_hbm, kb.at[b], lsem.at[0]),
        pltpu.make_async_copy(v_hbm, vb.at[b], lsem.at[1]),
        pltpu.make_async_copy(p_hbm, wp.at[z], lsem.at[2]),
        pltpu.make_async_copy(c_hbm, wc.at[z], lsem.at[3]),
        pltpu.make_async_copy(q_hbm, q, lsem.at[4]),
        pltpu.make_async_copy(r_hbm, res, lsem.at[5]),
    ]
    for copy in locals_:
        copy.start()

    barrier = pltpu.get_barrier_semaphore()

    def hello(where):
        pl.semaphore_signal(barrier, inc=1, device_id=where, device_id_type=MESH)

    for i in range(1, G):
        hello({"groups": lax.rem(g + i, G)})
    for i in range(1, X):
        hello({"blk": lax.rem(x + i, X) * 2 + c})
    hello({"blk": mate})
    pl.when(z > 0)(lambda: hello({"batch": z - 1}))
    pl.when(z < Z - 1)(lambda: hello({"batch": z + 1}))
    pl.when(b > 0)(lambda: hello({"blk": b - 1}))
    pl.when(b < B - 1)(lambda: hello({"blk": b + 1}))
    inner = (
        jnp.where(z > 0, 1, 0) + jnp.where(z < Z - 1, 1, 0)
        + jnp.where(b > 0, 1, 0) + jnp.where(b < B - 1, 1, 0)
    )
    pl.semaphore_wait(barrier, G - 1 + X - 1 + 1 + inner)

    def remote(ref, send, recv, where):
        return pltpu.make_async_remote_copy(
            src_ref=ref, dst_ref=ref, send_sem=send, recv_sem=recv,
            device_id=where, device_id_type=MESH,
        )

    kv = (kb, vb)

    def kv_out(w, i):
        return remote(kv[w].at[b], ksend.at[w, i], krecv.at[w, b // 2],
                      {"blk": lax.rem(x + i, X) * 2 + c})

    def kv_in(w, i):
        src = lax.rem(x + X - i, X)
        return remote(kv[w].at[src * 2 + c], ksend.at[w, i], krecv.at[w, src], {"blk": src * 2 + c})

    def kv_mate(w, i):
        src = lax.rem(x + X - i, X)
        return remote(kv[w].at[src * 2 + c], kcs.at[w, i], kcr.at[w, i], {"blk": mate})

    def kv_mate_in(w, i):
        src = lax.rem(x + X - i, X)
        return remote(kv[w].at[src * 2 + 1 - c], kcs.at[w, i], kcr.at[w, i], {"blk": mate})

    def item(j, s, p):
        if j == 0:
            return wp.at[s, pl.ds(pl.multiple_of(p * PP, 16), PP)]
        return wc.at[s, pl.ds(pl.multiple_of(p * PC + (j - 1) * CC, 16), CC)]

    mine = g * 2 + c

    def up(j, s):
        return remote(item(j, s, mine), zup.at[s, j], zrecv.at[s, j], {"batch": z + 1})

    def down(j, s):
        return remote(item(j, s, mine), zdn.at[s, j], zrecv.at[s, j], {"batch": z - 1})

    def side(j, s, i):
        return remote(item(j, s, mine), ysend.at[i, s, j], yrecv.at[i, s, j],
                      {"groups": lax.rem(g + i, G)})

    def side_in(j, s, i):
        other = lax.rem(g + G - i, G)
        return remote(item(j, s, other * 2 + c), ysend.at[i, s, j], yrecv.at[i, s, j],
                      {"groups": other})

    def cross(j, s, i):
        other = lax.rem(g + G - i, G)
        return remote(item(j, s, other * 2 + c), csend.at[i, s, j], crecv.at[i, s, j], {"blk": mate})

    def cross_in(j, s, i):
        other = lax.rem(g + G - i, G)
        return remote(item(j, s, other * 2 + 1 - c), csend.at[i, s, j], crecv.at[i, s, j], {"blk": mate})

    for w in range(2):
        locals_[w].wait()
        for i in range(1, X):
            kv_out(w, i).start()
        kv_mate(w, 0).start()
    locals_[2].wait()
    locals_[3].wait()
    for j in range(NI):
        pl.when(z < Z - 1)(lambda j=j: up(j, z).start())
        pl.when(z > 0)(lambda j=j: down(j, z).start())

    def arrived(j, d):
        @pl.when(z >= d)
        def _():
            s = z - d
            up(j, s).wait_recv()
            pl.when(z < Z - 1)(lambda: up(j, s).start())
            for i in range(1, G):
                side(j, s, i).start()
            cross(j, s, 0).start()

        @pl.when(z + d < Z)
        def _():
            s = z + d
            down(j, s).wait_recv()
            pl.when(z > 0)(lambda: down(j, s).start())
            for i in range(1, G):
                side(j, s, i).start()
            cross(j, s, 0).start()

    def relayed(j, d):
        for ok, s in ((z >= d, z - d), (z + d < Z, z + d)):
            @pl.when(ok)
            def _(s=s):
                for i in range(1, G):
                    side_in(j, s, i).wait_recv()
                    cross(j, s, i).start()

    def kv_pass(w):
        for i in range(1, X):
            kv_in(w, i).wait_recv()
            kv_mate(w, i).start()

    for d in range(1, Z):
        arrived(0, d)
    kv_pass(0)
    for j in range(1, NI):
        arrived(j, 1)
    kv_pass(1)
    for d in range(1, Z):
        relayed(0, d)
    for w in range(2):
        for i in range(X):
            kv_mate_in(w, i).wait_recv()
    locals_[4].wait()
    locals_[5].wait()

    first = lax.broadcasted_iota(jnp.int32, (1, 2 * HD), 1) < HD

    def pair(n, carry):
        cols = pl.ds(pl.multiple_of(n * 2 * HD, 2 * HD), 2 * HD)
        q2 = q[:, cols]
        outs = []
        for half in range(2):
            keep = first if half == 0 else jnp.logical_not(first)
            qh = jnp.where(keep, q2, jnp.zeros_like(q2))
            scores = [
                lax.dot_general(qh, kb[t, :, cols], (((1,), (1,)), ((), ())),
                                preferred_element_type=jnp.float32) * HD ** (-0.5)
                for t in range(B)
            ]
            top = functools.reduce(jnp.maximum, [jnp.max(s, axis=1, keepdims=True) for s in scores])
            total = jnp.zeros_like(top)
            mixed = jnp.zeros((T, 2 * HD), jnp.float32)
            for t in range(B):
                weights = jnp.exp(scores[t] - top)
                total = total + jnp.sum(weights, axis=1, keepdims=True)
                mixed = mixed + jnp.dot(weights.astype(jnp.bfloat16), vb[t, :, cols],
                                        preferred_element_type=jnp.float32)
            outs.append(mixed / total)
        att[:, cols] = jnp.where(first, outs[0], outs[1]).astype(jnp.bfloat16)
        return carry

    half_pairs = HEADS // 4
    lax.fori_loop(0, half_pairs, pair, 0)
    if Z > 2:
        arrived(1, 2)
    lax.fori_loop(half_pairs, HEADS // 2, pair, 0)
    if Z > 2:
        for j in range(2, NI):
            arrived(j, 2)
    for j in range(1, NI):
        relayed(j, 1)

    for d in range(1, Z):
        for ok, s in ((z >= d, z - d), (z + d < Z, z + d)):
            @pl.when(ok)
            def _(s=s):
                for i in range(G):
                    cross_in(0, s, i).wait_recv()
    own = BASE + COLS
    for s in range(Z):
        hidden = jnp.dot(att[...], wp[s], preferred_element_type=jnp.float32)
        hidden = hidden + res[:, s * CI:(s + 1) * CI].astype(jnp.float32)
        hidden = hidden.astype(jnp.bfloat16)
        wide = hidden.astype(jnp.float32)
        hext[s, own:own + T, :] = wide
        h_top[s] = hidden[:COLS]
        h_bot[s] = wide[T - COLS:].astype(jnp.bfloat16)

    def halo(src, dst, n, where):
        return pltpu.make_async_remote_copy(
            src_ref=src, dst_ref=dst, send_sem=hsend.at[n], recv_sem=hrecv.at[n],
            device_id={"blk": where}, device_id_type=MESH,
        )

    to_prev = lambda where: halo(h_top, r_bot, 0, where)
    to_next = lambda where: halo(h_bot, r_top, 1, where)
    pl.when(b > 0)(lambda: to_prev(b - 1).start())
    pl.when(b < B - 1)(lambda: to_next(b + 1).start())

    for d in range(3, Z):
        for j in range(1, NI):
            arrived(j, d)
            relayed(j, d - 1)
    if Z > 2:
        for j in range(1, NI):
            relayed(j, Z - 1)

    @pl.when(b > 0)
    def _():
        to_next(b - 1).wait_recv()
        for s in range(Z):
            hext[s, BASE:own, :] = r_top[s].astype(jnp.float32)

    @pl.when(b == 0)
    def _():
        for s in range(Z):
            hext[s, BASE:own, :] = jnp.zeros((COLS, CI), jnp.float32)

    @pl.when(b < B - 1)
    def _():
        to_prev(b + 1).wait_recv()
        for s in range(Z):
            hext[s, own + T:own + T + COLS, :] = r_bot[s].astype(jnp.float32)

    @pl.when(b == B - 1)
    def _():
        for s in range(Z):
            hext[s, own + T:own + T + COLS, :] = jnp.zeros((COLS, CI), jnp.float32)

    column = lax.rem(lax.broadcasted_iota(jnp.int32, (T, CI), 0), COLS)
    inside = (column != 0, None, column != COLS - 1)
    acc[...] = jnp.zeros_like(acc)

    def conv(n, carry):
        s = jnp.where(z * 2 < Z, lax.rem(z + n, Z), lax.rem(z - n + Z, Z))

        @pl.when(n > 0)
        def _():
            for j in range(1, NI):
                for i in range(G):
                    cross_in(j, s, i).wait_recv()

        total = acc[...]
        for row in range(3):
            for col in range(3):
                start = BASE + row * COLS + col - 1
                window = hext[s, start:start + T, :]
                if inside[col] is not None:
                    window = jnp.where(inside[col], window, 0.0)
                tap = row * 3 + col
                total = total + jnp.dot(window.astype(jnp.bfloat16), wc[s, tap * CI:(tap + 1) * CI, :],
                                        preferred_element_type=jnp.float32)
        acc[...] = total
        return carry

    lax.fori_loop(0, Z, conv, 0)
    o_ref[...] = acc[...].astype(jnp.bfloat16)

    for w in range(2):
        for i in range(1, X):
            kv_out(w, i).wait_send()
        for i in range(X):
            kv_mate(w, i).wait_send()
    pl.when(b > 0)(lambda: to_prev(b - 1).wait_send())
    pl.when(b < B - 1)(lambda: to_next(b + 1).wait_send())
    for j in range(NI):
        pl.when(z < Z - 1)(lambda j=j: up(j, z).wait_send())
        pl.when(z > 0)(lambda j=j: down(j, z).wait_send())
        for d in range(1, Z):
            @pl.when(z >= d)
            def _(j=j, d=d):
                pl.when(z < Z - 1)(lambda: up(j, z - d).wait_send())
                for i in range(1, G):
                    side(j, z - d, i).wait_send()
                for i in range(G):
                    cross(j, z - d, i).wait_send()

            @pl.when(z + d < Z)
            def _(j=j, d=d):
                pl.when(z > 0)(lambda: down(j, z + d).wait_send())
                for i in range(1, G):
                    side(j, z + d, i).wait_send()
                for i in range(G):
                    cross(j, z + d, i).wait_send()


def solution(mesh):
    G, Z, B = (mesh.shape[name] for name in ("groups", "batch", "blk"))

    def body(queries, key_states, value_states, residual, proj_weight, conv_weight):
        T = queries.shape[1]
        depth, CI = proj_weight.shape
        wide = residual.shape[2]
        taps = conv_weight.shape[0] * conv_weight.shape[1]
        out = conv_weight.shape[3]
        flat = conv_weight.reshape(taps * CI, out)
        unit = 2 * G * 16
        rows = -(-flat.shape[0] // unit) * unit
        if rows != flat.shape[0]:
            flat = jnp.pad(flat, ((0, rows - flat.shape[0]), (0, 0)))
        NC = 3 if (rows // unit) % 3 == 0 else 1
        NI = 1 + NC
        X = B // 2
        dma = pltpu.SemaphoreType.DMA
        bf16, f32 = jnp.bfloat16, jnp.float32
        result = pl.pallas_call(
            functools.partial(kernel, G, Z, B, CI, NC),
            out_shape=jax.ShapeDtypeStruct((T, out), bf16),
            in_specs=[pl.BlockSpec(memory_space=pl.ANY)] * 6,
            out_specs=pl.BlockSpec(memory_space=pltpu.VMEM),
            scratch_shapes=[
                pltpu.VMEM((T, depth), bf16),
                pltpu.VMEM((T, wide), bf16),
                pltpu.VMEM((B, T, depth), bf16),
                pltpu.VMEM((B, T, depth), bf16),
                pltpu.VMEM((Z, depth, CI), bf16),
                pltpu.VMEM((Z, rows, out), bf16),
                pltpu.VMEM((T, depth), bf16),
                pltpu.VMEM((Z, BASE + T + 2 * COLS + 8, CI), f32),
                pltpu.VMEM((Z, COLS, CI), bf16),
                pltpu.VMEM((Z, COLS, CI), bf16),
                pltpu.VMEM((Z, COLS, CI), bf16),
                pltpu.VMEM((Z, COLS, CI), bf16),
                pltpu.VMEM((T, out), f32),
                dma((6,)), dma((2, X)), dma((2, X)), dma((2, X)), dma((2, X)),
                dma((Z, NI)), dma((Z, NI)), dma((Z, NI)),
                dma((G, Z, NI)), dma((G, Z, NI)), dma((G, Z, NI)), dma((G, Z, NI)),
                dma((2,)), dma((2,)),
            ],
            compiler_params=pltpu.CompilerParams(
                collective_id=0, has_side_effects=True, vmem_limit_bytes=60 * 1024 * 1024
            ),
        )(queries[0], key_states[0], value_states[0], residual[0], proj_weight, flat)
        return result[None]

    return jax.shard_map(
        body,
        mesh=mesh,
        in_specs=(
            P(("groups", "batch"), "blk", None),
            P(("groups", "batch"), "blk", None),
            P(("groups", "batch"), "blk", None),
            P(("groups", "batch"), "blk", None),
            P(None, "batch"),
            P(None, None, "batch", None),
        ),
        out_specs=P(("groups", "batch"), "blk", None),
        check_vma=False,
    )
```

```python
import functools

import jax
import jax.numpy as jnp
from jax import lax
from jax.experimental import pallas as pl
from jax.experimental.pallas import tpu as pltpu
from jax.sharding import PartitionSpec as P

HEADS = 16
HD = 64
COLS = 74
BASE = 8
MESH = pl.DeviceIdType.MESH


def kernel(G, Z, B, CI, NC, q_hbm, k_hbm, v_hbm, r_hbm, p_hbm, c_hbm, o_ref,
           q, res, kb, vb, wp, wc, att, hext, h_top, h_bot, r_top, r_bot, acc,
           lsem, ksend, krecv, kcs, kcr, zup, zdn, zrecv, ysend, yrecv, csend, crecv, hsend, hrecv):
    T = q.shape[0]
    X = B // 2
    g = lax.axis_index("groups")
    z = lax.axis_index("batch")
    b = lax.axis_index("blk")
    c = lax.rem(b, 2)
    x = b // 2
    mate = x * 2 + 1 - c
    NI = 1 + NC
    PP = wp.shape[2] // (2 * G)
    PC = wc.shape[1] // (2 * G)
    CC = PC // NC

    locals_ = [
        pltpu.make_async_copy(k_hbm, kb.at[b], lsem.at[0]),
        pltpu.make_async_copy(v_hbm, vb.at[b], lsem.at[1]),
        pltpu.make_async_copy(p_hbm, wp.at[z], lsem.at[2]),
        pltpu.make_async_copy(c_hbm, wc.at[z], lsem.at[3]),
        pltpu.make_async_copy(q_hbm, q, lsem.at[4]),
        pltpu.make_async_copy(r_hbm, res, lsem.at[5]),
    ]
    for copy in locals_:
        copy.start()

    barrier = pltpu.get_barrier_semaphore()

    def hello(where):
        pl.semaphore_signal(barrier, inc=1, device_id=where, device_id_type=MESH)

    for i in range(1, G):
        hello({"groups": lax.rem(g + i, G)})
    for i in range(1, X):
        hello({"blk": lax.rem(x + i, X) * 2 + c})
    hello({"blk": mate})
    pl.when(z > 0)(lambda: hello({"batch": z - 1}))
    pl.when(z < Z - 1)(lambda: hello({"batch": z + 1}))
    pl.when(b > 0)(lambda: hello({"blk": b - 1}))
    pl.when(b < B - 1)(lambda: hello({"blk": b + 1}))
    inner = (
        jnp.where(z > 0, 1, 0) + jnp.where(z < Z - 1, 1, 0)
        + jnp.where(b > 0, 1, 0) + jnp.where(b < B - 1, 1, 0)
    )
    pl.semaphore_wait(barrier, G - 1 + X - 1 + 1 + inner)

    def remote(ref, send, recv, where):
        return pltpu.make_async_remote_copy(
            src_ref=ref, dst_ref=ref, send_sem=send, recv_sem=recv,
            device_id=where, device_id_type=MESH,
        )

    kv = (kb, vb)

    def kv_out(w, i):
        return remote(kv[w].at[b], ksend.at[w, i], krecv.at[w, b // 2],
                      {"blk": lax.rem(x + i, X) * 2 + c})

    def kv_in(w, i):
        src = lax.rem(x + X - i, X)
        return remote(kv[w].at[src * 2 + c], ksend.at[w, i], krecv.at[w, src], {"blk": src * 2 + c})

    def kv_mate(w, i):
        src = lax.rem(x + X - i, X)
        return remote(kv[w].at[src * 2 + c], kcs.at[w, i], kcr.at[w, i], {"blk": mate})

    def kv_mate_in(w, i):
        src = lax.rem(x + X - i, X)
        return remote(kv[w].at[src * 2 + 1 - c], kcs.at[w, i], kcr.at[w, i], {"blk": mate})

    def item(j, s, p):
        if j == 0:
            return wp.at[s, :, pl.ds(pl.multiple_of(p * PP, 128), PP)]
        return wc.at[s, pl.ds(pl.multiple_of(p * PC + (j - 1) * CC, 16), CC)]

    mine = g * 2 + c

    def up(j, s):
        return remote(item(j, s, mine), zup.at[s, j], zrecv.at[s, j], {"batch": z + 1})

    def down(j, s):
        return remote(item(j, s, mine), zdn.at[s, j], zrecv.at[s, j], {"batch": z - 1})

    def side(j, s, i):
        return remote(item(j, s, mine), ysend.at[i, s, j], yrecv.at[i, s, j],
                      {"groups": lax.rem(g + i, G)})

    def side_in(j, s, i):
        other = lax.rem(g + G - i, G)
        return remote(item(j, s, other * 2 + c), ysend.at[i, s, j], yrecv.at[i, s, j],
                      {"groups": other})

    def cross(j, s, i):
        other = lax.rem(g + G - i, G)
        return remote(item(j, s, other * 2 + c), csend.at[i, s, j], crecv.at[i, s, j], {"blk": mate})

    def cross_in(j, s, i):
        other = lax.rem(g + G - i, G)
        return remote(item(j, s, other * 2 + 1 - c), csend.at[i, s, j], crecv.at[i, s, j], {"blk": mate})

    for w in range(2):
        locals_[w].wait()
        for i in range(1, X):
            kv_out(w, i).start()
        kv_mate(w, 0).start()
    def launch(j):
        pl.when(z < Z - 1)(lambda: up(j, z).start())
        pl.when(z > 0)(lambda: down(j, z).start())

    def arrived(j, d):
        @pl.when(z >= d)
        def _():
            s = z - d
            up(j, s).wait_recv()
            pl.when(z < Z - 1)(lambda: up(j, s).start())
            for i in range(1, G):
                side(j, s, i).start()
            cross(j, s, 0).start()

        @pl.when(z + d < Z)
        def _():
            s = z + d
            down(j, s).wait_recv()
            pl.when(z > 0)(lambda: down(j, s).start())
            for i in range(1, G):
                side(j, s, i).start()
            cross(j, s, 0).start()

    def relayed(j, d):
        for ok, s in ((z >= d, z - d), (z + d < Z, z + d)):
            @pl.when(ok)
            def _(s=s):
                for i in range(1, G):
                    side_in(j, s, i).wait_recv()
                    cross(j, s, i).start()

    def kv_pass(w):
        for i in range(1, X):
            kv_in(w, i).wait_recv()
            kv_mate(w, i).start()

    locals_[2].wait()
    launch(0)
    locals_[3].wait()
    launch(1)
    arrived(0, 1)
    for j in range(2, NI):
        launch(j)
        if j < Z:
            arrived(0, j)
        arrived(j - 1, 1)
    kv_pass(0)
    for d in range(max(NI, 2), Z):
        arrived(0, d)
    arrived(NI - 1, 1)
    kv_pass(1)
    for d in range(1, min(3, Z)):
        relayed(0, d)
    for w in range(2):
        for i in range(X):
            kv_mate_in(w, i).wait_recv()
    locals_[4].wait()
    locals_[5].wait()

    first = lax.broadcasted_iota(jnp.int32, (1, 2 * HD), 1) < HD

    def pair(n, carry):
        cols = pl.ds(pl.multiple_of(n * 2 * HD, 2 * HD), 2 * HD)
        q2 = q[:, cols]
        outs = []
        for half in range(2):
            keep = first if half == 0 else jnp.logical_not(first)
            qh = jnp.where(keep, q2, jnp.zeros_like(q2))
            scores = [
                lax.dot_general(qh, kb[t, :, cols], (((1,), (1,)), ((), ())),
                                preferred_element_type=jnp.float32) * HD ** (-0.5)
                for t in range(B)
            ]
            top = functools.reduce(jnp.maximum, [jnp.max(s, axis=1, keepdims=True) for s in scores])
            total = jnp.zeros_like(top)
            mixed = jnp.zeros((T, 2 * HD), jnp.float32)
            for t in range(B):
                weights = jnp.exp(scores[t] - top)
                total = total + jnp.sum(weights, axis=1, keepdims=True)
                mixed = mixed + jnp.dot(weights.astype(jnp.bfloat16), vb[t, :, cols],
                                        preferred_element_type=jnp.float32)
            outs.append(mixed / total)
        att[:, cols] = jnp.where(first, outs[0], outs[1]).astype(jnp.bfloat16)
        return carry

    half_pairs = HEADS // 4
    lax.fori_loop(0, half_pairs, pair, 0)
    if Z > 2:
        arrived(1, 2)
    lax.fori_loop(half_pairs, HEADS // 2, pair, 0)
    if Z > 2:
        for j in range(2, NI):
            arrived(j, 2)
    for d in range(3, Z):
        relayed(0, d)
    for j in range(1, NI):
        relayed(j, 1)

    for d in range(1, Z):
        for ok, s in ((z >= d, z - d), (z + d < Z, z + d)):
            @pl.when(ok)
            def _(s=s):
                for i in range(G):
                    cross_in(0, s, i).wait_recv()
    own = BASE + COLS
    for s in range(Z):
        hidden = lax.dot_general(att[...], wp[s], (((1,), (1,)), ((), ())),
                                 preferred_element_type=jnp.float32)
        hidden = hidden + res[:, s * CI:(s + 1) * CI].astype(jnp.float32)
        hidden = hidden.astype(jnp.bfloat16)
        wide = hidden.astype(jnp.float32)
        hext[s, own:own + T, :] = wide
        h_top[s] = hidden[:COLS]
        h_bot[s] = wide[T - COLS:].astype(jnp.bfloat16)

    def halo(src, dst, n, where):
        return pltpu.make_async_remote_copy(
            src_ref=src, dst_ref=dst, send_sem=hsend.at[n], recv_sem=hrecv.at[n],
            device_id={"blk": where}, device_id_type=MESH,
        )

    to_prev = lambda where: halo(h_top, r_bot, 0, where)
    to_next = lambda where: halo(h_bot, r_top, 1, where)
    pl.when(b > 0)(lambda: to_prev(b - 1).start())
    pl.when(b < B - 1)(lambda: to_next(b + 1).start())

    @pl.when(b > 0)
    def _():
        to_next(b - 1).wait_recv()
        for s in range(Z):
            hext[s, BASE:own, :] = r_top[s].astype(jnp.float32)

    @pl.when(b == 0)
    def _():
        for s in range(Z):
            hext[s, BASE:own, :] = jnp.zeros((COLS, CI), jnp.float32)

    @pl.when(b < B - 1)
    def _():
        to_prev(b + 1).wait_recv()
        for s in range(Z):
            hext[s, own + T:own + T + COLS, :] = r_bot[s].astype(jnp.float32)

    @pl.when(b == B - 1)
    def _():
        for s in range(Z):
            hext[s, own + T:own + T + COLS, :] = jnp.zeros((COLS, CI), jnp.float32)

    column = lax.rem(lax.broadcasted_iota(jnp.int32, (T, CI), 0), COLS)
    inside = (column != 0, None, column != COLS - 1)
    acc[...] = jnp.zeros_like(acc)

    def conv(n):
        s = jnp.where(z * 2 < Z, lax.rem(z + n, Z), lax.rem(z - n + Z, Z))

        if n > 0:
            for j in range(1, NI):
                for i in range(G):
                    cross_in(j, s, i).wait_recv()
        total = acc[...]
        for row in range(3):
            for col in range(3):
                start = BASE + row * COLS + col - 1
                window = hext[s, start:start + T, :]
                if inside[col] is not None:
                    window = jnp.where(inside[col], window, 0.0)
                tap = row * 3 + col
                total = total + jnp.dot(window.astype(jnp.bfloat16), wc[s, tap * CI:(tap + 1) * CI, :],
                                        preferred_element_type=jnp.float32)
        acc[...] = total

    for n in range(Z):
        conv(n)
        if n > 0:
            for j in range(2, NI):
                if n + 1 < Z:
                    relayed(j, n + 1)
                if n + 2 < Z:
                    arrived(j, n + 2)
        if n + 3 < Z:
            arrived(1, n + 3)
        if n + 2 < Z:
            relayed(1, n + 2)
    o_ref[...] = acc[...].astype(jnp.bfloat16)

    for w in range(2):
        for i in range(1, X):
            kv_out(w, i).wait_send()
        for i in range(X):
            kv_mate(w, i).wait_send()
    pl.when(b > 0)(lambda: to_prev(b - 1).wait_send())
    pl.when(b < B - 1)(lambda: to_next(b + 1).wait_send())
    for j in range(NI):
        pl.when(z < Z - 1)(lambda j=j: up(j, z).wait_send())
        pl.when(z > 0)(lambda j=j: down(j, z).wait_send())
        for d in range(1, Z):
            @pl.when(z >= d)
            def _(j=j, d=d):
                pl.when(z < Z - 1)(lambda: up(j, z - d).wait_send())
                for i in range(1, G):
                    side(j, z - d, i).wait_send()
                for i in range(G):
                    cross(j, z - d, i).wait_send()

            @pl.when(z + d < Z)
            def _(j=j, d=d):
                pl.when(z > 0)(lambda: down(j, z + d).wait_send())
                for i in range(1, G):
                    side(j, z + d, i).wait_send()
                for i in range(G):
                    cross(j, z + d, i).wait_send()


def solution(mesh):
    G, Z, B = (mesh.shape[name] for name in ("groups", "batch", "blk"))

    def body(queries, key_states, value_states, residual, proj_weight, conv_weight):
        T = queries.shape[1]
        depth, CI = proj_weight.shape
        wide = residual.shape[2]
        taps = conv_weight.shape[0] * conv_weight.shape[1]
        out = conv_weight.shape[3]
        flat = conv_weight.reshape(taps * CI, out)
        unit = 2 * G * 16
        rows = -(-flat.shape[0] // unit) * unit
        if rows != flat.shape[0]:
            flat = jnp.pad(flat, ((0, rows - flat.shape[0]), (0, 0)))
        NC = 3 if (rows // unit) % 3 == 0 else 1
        NI = 1 + NC
        X = B // 2
        dma = pltpu.SemaphoreType.DMA
        bf16, f32 = jnp.bfloat16, jnp.float32
        result = pl.pallas_call(
            functools.partial(kernel, G, Z, B, CI, NC),
            out_shape=jax.ShapeDtypeStruct((T, out), bf16),
            in_specs=[pl.BlockSpec(memory_space=pl.ANY)] * 6,
            out_specs=pl.BlockSpec(memory_space=pltpu.VMEM),
            scratch_shapes=[
                pltpu.VMEM((T, depth), bf16),
                pltpu.VMEM((T, wide), bf16),
                pltpu.VMEM((B, T, depth), bf16),
                pltpu.VMEM((B, T, depth), bf16),
                pltpu.VMEM((Z, CI, depth), bf16),
                pltpu.VMEM((Z, rows, out), bf16),
                pltpu.VMEM((T, depth), bf16),
                pltpu.VMEM((Z, BASE + T + 2 * COLS + 8, CI), f32),
                pltpu.VMEM((Z, COLS, CI), bf16),
                pltpu.VMEM((Z, COLS, CI), bf16),
                pltpu.VMEM((Z, COLS, CI), bf16),
                pltpu.VMEM((Z, COLS, CI), bf16),
                pltpu.VMEM((T, out), f32),
                dma((6,)), dma((2, X)), dma((2, X)), dma((2, X)), dma((2, X)),
                dma((Z, NI)), dma((Z, NI)), dma((Z, NI)),
                dma((G, Z, NI)), dma((G, Z, NI)), dma((G, Z, NI)), dma((G, Z, NI)),
                dma((2,)), dma((2,)),
            ],
            compiler_params=pltpu.CompilerParams(
                collective_id=0, has_side_effects=True, vmem_limit_bytes=60 * 1024 * 1024
            ),
        )(queries[0], key_states[0], value_states[0], residual[0], proj_weight.T, flat)
        return result[None]

    return jax.shard_map(
        body,
        mesh=mesh,
        in_specs=(
            P(("groups", "batch"), "blk", None),
            P(("groups", "batch"), "blk", None),
            P(("groups", "batch"), "blk", None),
            P(("groups", "batch"), "blk", None),
            P(None, "batch"),
            P(None, None, "batch", None),
        ),
        out_specs=P(("groups", "batch"), "blk", None),
        check_vma=False,
    )
```

```python
import functools

import jax
import jax.numpy as jnp
from jax import lax
from jax.experimental import pallas as pl
from jax.experimental.pallas import tpu as pltpu
from jax.sharding import PartitionSpec as P

HEADS = 16
HD = 64
COLS = 74
BASE = 8
MESH = pl.DeviceIdType.MESH


def kernel(G, Z, B, CI, NC, q_hbm, k_hbm, v_hbm, r_hbm, p_hbm, c_hbm, o_ref,
           q, res, kb, vb, wp, wc, att, hext, h_top, h_bot, r_top, r_bot, acc,
           lsem, ksend, krecv, kcs, kcr, zup, zdn, zrecv, ysend, yrecv, csend, crecv, hsend, hrecv):
    T = q.shape[0]
    X = B // 2
    g = lax.axis_index("groups")
    z = lax.axis_index("batch")
    b = lax.axis_index("blk")
    c = lax.rem(b, 2)
    x = b // 2
    mate = x * 2 + 1 - c
    NI = 1 + NC
    PP = wp.shape[2] // (2 * G)
    PC = wc.shape[1] // (2 * G)
    CC = PC // NC

    locals_ = [
        pltpu.make_async_copy(k_hbm, kb.at[b], lsem.at[0]),
        pltpu.make_async_copy(v_hbm, vb.at[b], lsem.at[1]),
        pltpu.make_async_copy(p_hbm, wp.at[z], lsem.at[2]),
        pltpu.make_async_copy(c_hbm, wc.at[z], lsem.at[3]),
        pltpu.make_async_copy(q_hbm, q, lsem.at[4]),
        pltpu.make_async_copy(r_hbm, res, lsem.at[5]),
    ]
    for copy in locals_:
        copy.start()

    barrier = pltpu.get_barrier_semaphore()

    def hello(where):
        pl.semaphore_signal(barrier, inc=1, device_id=where, device_id_type=MESH)

    for i in range(1, G):
        hello({"groups": lax.rem(g + i, G)})
    for i in range(1, X):
        hello({"blk": lax.rem(x + i, X) * 2 + c})
    hello({"blk": mate})
    pl.when(z > 0)(lambda: hello({"batch": z - 1}))
    pl.when(z < Z - 1)(lambda: hello({"batch": z + 1}))
    pl.when(b > 0)(lambda: hello({"blk": b - 1}))
    pl.when(b < B - 1)(lambda: hello({"blk": b + 1}))
    inner = (
        jnp.where(z > 0, 1, 0) + jnp.where(z < Z - 1, 1, 0)
        + jnp.where(b > 0, 1, 0) + jnp.where(b < B - 1, 1, 0)
    )
    pl.semaphore_wait(barrier, G - 1 + X - 1 + 1 + inner)

    def remote(ref, send, recv, where):
        return pltpu.make_async_remote_copy(
            src_ref=ref, dst_ref=ref, send_sem=send, recv_sem=recv,
            device_id=where, device_id_type=MESH,
        )

    kv = (kb, vb)

    def kv_out(w, i):
        return remote(kv[w].at[b], ksend.at[w, i], krecv.at[w, b // 2],
                      {"blk": lax.rem(x + i, X) * 2 + c})

    def kv_in(w, i):
        src = lax.rem(x + X - i, X)
        return remote(kv[w].at[src * 2 + c], ksend.at[w, i], krecv.at[w, src], {"blk": src * 2 + c})

    def kv_mate(w, i):
        src = lax.rem(x + X - i, X)
        return remote(kv[w].at[src * 2 + c], kcs.at[w, i], kcr.at[w, i], {"blk": mate})

    def kv_mate_in(w, i):
        src = lax.rem(x + X - i, X)
        return remote(kv[w].at[src * 2 + 1 - c], kcs.at[w, i], kcr.at[w, i], {"blk": mate})

    def item(j, s, p):
        if j == 0:
            return wp.at[s, :, pl.ds(pl.multiple_of(p * PP, 128), PP)]
        return wc.at[s, pl.ds(pl.multiple_of(p * PC + (j - 1) * CC, 16), CC)]

    def along_x(j):
        return X == G and NI > 2 and j == NI - 1

    def place(j):
        return x if along_x(j) else g

    def peer(j, n):
        return {"blk": n * 2 + c} if along_x(j) else {"groups": n}


    def up(j, s):
        return remote(item(j, s, place(j) * 2 + c), zup.at[s, j], zrecv.at[s, j], {"batch": z + 1})

    def down(j, s):
        return remote(item(j, s, place(j) * 2 + c), zdn.at[s, j], zrecv.at[s, j], {"batch": z - 1})

    def side(j, s, i):
        return remote(item(j, s, place(j) * 2 + c), ysend.at[i, s, j], yrecv.at[i, s, j],
                      peer(j, lax.rem(place(j) + i, G)))

    def side_in(j, s, i):
        other = lax.rem(place(j) + G - i, G)
        return remote(item(j, s, other * 2 + c), ysend.at[i, s, j], yrecv.at[i, s, j],
                      peer(j, other))

    def cross(j, s, i):
        other = lax.rem(place(j) + G - i, G)
        return remote(item(j, s, other * 2 + c), csend.at[i, s, j], crecv.at[i, s, j], {"blk": mate})

    def cross_in(j, s, i):
        other = lax.rem(place(j) + G - i, G)
        return remote(item(j, s, other * 2 + 1 - c), csend.at[i, s, j], crecv.at[i, s, j], {"blk": mate})

    for w in range(2):
        locals_[w].wait()
        for i in range(1, X):
            kv_out(w, i).start()
        kv_mate(w, 0).start()
    def launch(j):
        pl.when(z < Z - 1)(lambda: up(j, z).start())
        pl.when(z > 0)(lambda: down(j, z).start())

    def arrived(j, d):
        @pl.when(z >= d)
        def _():
            s = z - d
            up(j, s).wait_recv()
            pl.when(z < Z - 1)(lambda: up(j, s).start())
            for i in range(1, G):
                side(j, s, i).start()
            cross(j, s, 0).start()

        @pl.when(z + d < Z)
        def _():
            s = z + d
            down(j, s).wait_recv()
            pl.when(z > 0)(lambda: down(j, s).start())
            for i in range(1, G):
                side(j, s, i).start()
            cross(j, s, 0).start()

    def relayed(j, d):
        for ok, s in ((z >= d, z - d), (z + d < Z, z + d)):
            @pl.when(ok)
            def _(s=s):
                for i in range(1, G):
                    side_in(j, s, i).wait_recv()
                    cross(j, s, i).start()

    def kv_pass(w):
        for i in range(1, X):
            kv_in(w, i).wait_recv()
            kv_mate(w, i).start()

    locals_[2].wait()
    launch(0)
    locals_[3].wait()
    launch(1)
    arrived(0, 1)
    for j in range(2, NI):
        launch(j)
        if j < Z:
            arrived(0, j)
        arrived(j - 1, 1)
    kv_pass(0)
    for d in range(max(NI, 2), Z):
        arrived(0, d)
    arrived(NI - 1, 1)
    kv_pass(1)
    for d in range(1, min(3, Z)):
        relayed(0, d)
    for w in range(2):
        for i in range(X):
            kv_mate_in(w, i).wait_recv()
    locals_[4].wait()
    locals_[5].wait()

    first = lax.broadcasted_iota(jnp.int32, (1, 2 * HD), 1) < HD

    def pair(n, carry):
        cols = pl.ds(pl.multiple_of(n * 2 * HD, 2 * HD), 2 * HD)
        q2 = q[:, cols]
        outs = []
        for half in range(2):
            keep = first if half == 0 else jnp.logical_not(first)
            qh = jnp.where(keep, q2, jnp.zeros_like(q2))
            scores = [
                lax.dot_general(qh, kb[t, :, cols], (((1,), (1,)), ((), ())),
                                preferred_element_type=jnp.float32) * HD ** (-0.5)
                for t in range(B)
            ]
            top = functools.reduce(jnp.maximum, [jnp.max(s, axis=1, keepdims=True) for s in scores])
            total = jnp.zeros_like(top)
            mixed = jnp.zeros((T, 2 * HD), jnp.float32)
            for t in range(B):
                weights = jnp.exp(scores[t] - top)
                total = total + jnp.sum(weights, axis=1, keepdims=True)
                mixed = mixed + jnp.dot(weights.astype(jnp.bfloat16), vb[t, :, cols],
                                        preferred_element_type=jnp.float32)
            outs.append(mixed / total)
        att[:, cols] = jnp.where(first, outs[0], outs[1]).astype(jnp.bfloat16)
        return carry

    half_pairs = HEADS // 4
    lax.fori_loop(0, half_pairs, pair, 0)
    if Z > 2:
        arrived(1, 2)
    lax.fori_loop(half_pairs, HEADS // 2, pair, 0)
    if Z > 2:
        for j in range(2, NI):
            arrived(j, 2)
    for d in range(3, Z):
        relayed(0, d)
    for j in range(1, NI):
        relayed(j, 1)

    for d in range(1, Z):
        for ok, s in ((z >= d, z - d), (z + d < Z, z + d)):
            @pl.when(ok)
            def _(s=s):
                for i in range(G):
                    cross_in(0, s, i).wait_recv()
    own = BASE + COLS
    for s in range(Z):
        hidden = lax.dot_general(att[...], wp[s], (((1,), (1,)), ((), ())),
                                 preferred_element_type=jnp.float32)
        hidden = hidden + res[:, s * CI:(s + 1) * CI].astype(jnp.float32)
        hidden = hidden.astype(jnp.bfloat16)
        wide = hidden.astype(jnp.float32)
        hext[s, own:own + T, :] = wide
        h_top[s] = hidden[:COLS]
        h_bot[s] = wide[T - COLS:].astype(jnp.bfloat16)

    def halo(src, dst, n, where):
        return pltpu.make_async_remote_copy(
            src_ref=src, dst_ref=dst, send_sem=hsend.at[n], recv_sem=hrecv.at[n],
            device_id={"blk": where}, device_id_type=MESH,
        )

    to_prev = lambda where: halo(h_top, r_bot, 0, where)
    to_next = lambda where: halo(h_bot, r_top, 1, where)
    pl.when(b > 0)(lambda: to_prev(b - 1).start())
    pl.when(b < B - 1)(lambda: to_next(b + 1).start())

    @pl.when(b > 0)
    def _():
        to_next(b - 1).wait_recv()
        for s in range(Z):
            hext[s, BASE:own, :] = r_top[s].astype(jnp.float32)

    @pl.when(b == 0)
    def _():
        for s in range(Z):
            hext[s, BASE:own, :] = jnp.zeros((COLS, CI), jnp.float32)

    @pl.when(b < B - 1)
    def _():
        to_prev(b + 1).wait_recv()
        for s in range(Z):
            hext[s, own + T:own + T + COLS, :] = r_bot[s].astype(jnp.float32)

    @pl.when(b == B - 1)
    def _():
        for s in range(Z):
            hext[s, own + T:own + T + COLS, :] = jnp.zeros((COLS, CI), jnp.float32)

    column = lax.rem(lax.broadcasted_iota(jnp.int32, (T, CI), 0), COLS)
    inside = (column != 0, None, column != COLS - 1)
    acc[...] = jnp.zeros_like(acc)

    def conv(n):
        s = jnp.where(z * 2 < Z, lax.rem(z + n, Z), lax.rem(z - n + Z, Z))

        if n > 0:
            for j in range(1, NI):
                for i in range(G):
                    cross_in(j, s, i).wait_recv()
        total = acc[...]
        for row in range(3):
            for col in range(3):
                start = BASE + row * COLS + col - 1
                window = hext[s, start:start + T, :]
                if inside[col] is not None:
                    window = jnp.where(inside[col], window, 0.0)
                tap = row * 3 + col
                total = total + jnp.dot(window.astype(jnp.bfloat16), wc[s, tap * CI:(tap + 1) * CI, :],
                                        preferred_element_type=jnp.float32)
        acc[...] = total

    for n in range(Z):
        conv(n)
        if n > 0:
            for j in range(2, NI):
                if n + 1 < Z:
                    relayed(j, n + 1)
                if n + 2 < Z:
                    arrived(j, n + 2)
        if n + 3 < Z:
            arrived(1, n + 3)
        if n + 2 < Z:
            relayed(1, n + 2)
    o_ref[...] = acc[...].astype(jnp.bfloat16)

    for w in range(2):
        for i in range(1, X):
            kv_out(w, i).wait_send()
        for i in range(X):
            kv_mate(w, i).wait_send()
    pl.when(b > 0)(lambda: to_prev(b - 1).wait_send())
    pl.when(b < B - 1)(lambda: to_next(b + 1).wait_send())
    for j in range(NI):
        pl.when(z < Z - 1)(lambda j=j: up(j, z).wait_send())
        pl.when(z > 0)(lambda j=j: down(j, z).wait_send())
        for d in range(1, Z):
            @pl.when(z >= d)
            def _(j=j, d=d):
                pl.when(z < Z - 1)(lambda: up(j, z - d).wait_send())
                for i in range(1, G):
                    side(j, z - d, i).wait_send()
                for i in range(G):
                    cross(j, z - d, i).wait_send()

            @pl.when(z + d < Z)
            def _(j=j, d=d):
                pl.when(z > 0)(lambda: down(j, z + d).wait_send())
                for i in range(1, G):
                    side(j, z + d, i).wait_send()
                for i in range(G):
                    cross(j, z + d, i).wait_send()


def solution(mesh):
    G, Z, B = (mesh.shape[name] for name in ("groups", "batch", "blk"))

    def body(queries, key_states, value_states, residual, proj_weight, conv_weight):
        T = queries.shape[1]
        depth, CI = proj_weight.shape
        wide = residual.shape[2]
        taps = conv_weight.shape[0] * conv_weight.shape[1]
        out = conv_weight.shape[3]
        flat = conv_weight.reshape(taps * CI, out)
        unit = 2 * G * 16
        rows = -(-flat.shape[0] // unit) * unit
        if rows != flat.shape[0]:
            flat = jnp.pad(flat, ((0, rows - flat.shape[0]), (0, 0)))
        NC = 3 if (rows // unit) % 3 == 0 else 1
        NI = 1 + NC
        X = B // 2
        dma = pltpu.SemaphoreType.DMA
        bf16, f32 = jnp.bfloat16, jnp.float32
        result = pl.pallas_call(
            functools.partial(kernel, G, Z, B, CI, NC),
            out_shape=jax.ShapeDtypeStruct((T, out), bf16),
            in_specs=[pl.BlockSpec(memory_space=pl.ANY)] * 6,
            out_specs=pl.BlockSpec(memory_space=pltpu.VMEM),
            scratch_shapes=[
                pltpu.VMEM((T, depth), bf16),
                pltpu.VMEM((T, wide), bf16),
                pltpu.VMEM((B, T, depth), bf16),
                pltpu.VMEM((B, T, depth), bf16),
                pltpu.VMEM((Z, CI, depth), bf16),
                pltpu.VMEM((Z, rows, out), bf16),
                pltpu.VMEM((T, depth), bf16),
                pltpu.VMEM((Z, BASE + T + 2 * COLS + 8, CI), f32),
                pltpu.VMEM((Z, COLS, CI), bf16),
                pltpu.VMEM((Z, COLS, CI), bf16),
                pltpu.VMEM((Z, COLS, CI), bf16),
                pltpu.VMEM((Z, COLS, CI), bf16),
                pltpu.VMEM((T, out), f32),
                dma((6,)), dma((2, X)), dma((2, X)), dma((2, X)), dma((2, X)),
                dma((Z, NI)), dma((Z, NI)), dma((Z, NI)),
                dma((G, Z, NI)), dma((G, Z, NI)), dma((G, Z, NI)), dma((G, Z, NI)),
                dma((2,)), dma((2,)),
            ],
            compiler_params=pltpu.CompilerParams(
                collective_id=0, has_side_effects=True, vmem_limit_bytes=60 * 1024 * 1024
            ),
        )(queries[0], key_states[0], value_states[0], residual[0], proj_weight.T, flat)
        return result[None]

    return jax.shard_map(
        body,
        mesh=mesh,
        in_specs=(
            P(("groups", "batch"), "blk", None),
            P(("groups", "batch"), "blk", None),
            P(("groups", "batch"), "blk", None),
            P(("groups", "batch"), "blk", None),
            P(None, "batch"),
            P(None, None, "batch", None),
        ),
        out_specs=P(("groups", "batch"), "blk", None),
        check_vma=False,
    )
```
